8 devices in a mesh: fsdp: 2 (over z, y), model: 4 (over x, core).
Axes of the slice: x: 2, y: 2, z: 1, core: 2. Of those that a mesh axis runs over, the one named last changes fastest.
Arguments:
- x_in: bfloat16 [4, 1024, 3584], P('fsdp', 'model')
- dy_in: bfloat16 [4, 1024, 3584], P('fsdp', 'model')
- norm_gain: float32 [3584], replicated
- w_qkv: bfloat16 [3584, 4608], P('fsdp', 'model')
- w_out: bfloat16 [3584, 3584], P('model', 'fsdp')
- w_gate: bfloat16 [3584, 18944], P('fsdp', 'model')
- w_up: bfloat16 [3584, 18944], P('fsdp', 'model')
- w_down: bfloat16 [18944, 3584], P('model', 'fsdp')
- rope_cos: float32 [1024, 64], replicated
- rope_sin: float32 [1024, 64], replicated
Outputs:
- output 1: bfloat16 [4, 1024, 3584], P('fsdp', 'model')
- output 2: bfloat16 [4, 1024, 3584], P('fsdp', 'model')
- output 3: float32 [3584, 4608], P('fsdp', 'model')
- output 4: float32 [3584, 3584], P('model', 'fsdp')
- output 5: float32 [3584, 18944], P('fsdp', 'model')
- output 6: float32 [3584, 18944], P('fsdp', 'model')
- output 7: float32 [18944, 3584], P('model', 'fsdp')
All inputs are finite; a program needn't handle non-finite values.
Results may differ from the reference program's by a relative error of at most 0.00910455.
Values are sent between devices in bfloat16 or wider.
A program may use at most 1 GiB of HBM per device.

```python
import math
import jax
import jax.numpy as jnp
from jax import lax

D = 3584
FF = 18944
HEADS = 28
KV_HEADS = 4
HEAD = 128
BATCH = 4
SEQ = 1024
ROPE_THETA = 500000

NORM_EPS = 1e-5
GROUP_SIZE = HEADS // KV_HEADS
QKV_COLS = (HEADS + 2 * KV_HEADS) * HEAD


def rope_tables(key):
    pos_gaps = jax.random.randint(key, (SEQ,), 1, 4)
    positions = (jnp.cumsum(pos_gaps) - pos_gaps[0]).astype(jnp.float32)
    inv_freq = jnp.exp(jnp.arange(HEAD // 2, dtype=jnp.float32) * (-2.0 * math.log(ROPE_THETA) / HEAD))
    angles = positions[:, None] * inv_freq[None, :]
    return jnp.cos(angles), jnp.sin(angles)


def setup_inputs(seed: int = 0) -> dict:
    key_list = jax.random.split(jax.random.key(seed), 9)
    x_in = jax.random.normal(key_list[0], (BATCH, SEQ, D), jnp.float32)
    dy_in = jax.random.normal(key_list[1], (BATCH, SEQ, D), jnp.float32)
    norm_gain = jax.random.uniform(key_list[2], (D,), jnp.float32, 0.5, 1.5)
    w_qkv = jax.random.normal(key_list[3], (D, QKV_COLS), jnp.float32) * D ** -0.5
    w_out = jax.random.normal(key_list[4], (HEADS * HEAD, D), jnp.float32) * (HEADS * HEAD) ** -0.5
    w_gate = jax.random.normal(key_list[5], (D, FF), jnp.float32) * D ** -0.5
    w_up = jax.random.normal(key_list[6], (D, FF), jnp.float32) * D ** -0.5
    w_down = jax.random.normal(key_list[7], (FF, D), jnp.float32) * FF ** -0.5
    rope_cos, rope_sin = rope_tables(key_list[8])
    return {
        "x_in": x_in.astype(jnp.bfloat16),
        "dy_in": dy_in.astype(jnp.bfloat16),
        "norm_gain": norm_gain,
        "w_qkv": w_qkv.astype(jnp.bfloat16),
        "w_out": w_out.astype(jnp.bfloat16),
        "w_gate": w_gate.astype(jnp.bfloat16),
        "w_up": w_up.astype(jnp.bfloat16),
        "w_down": w_down.astype(jnp.bfloat16),
        "rope_cos": rope_cos,
        "rope_sin": rope_sin,
    }


def rotate(tensor, cos_tab, sin_tab):
    half_dim = HEAD // 2
    wide = tensor.astype(jnp.float32)
    lower_half = wide[..., :half_dim]
    upper_half = wide[..., half_dim:]
    return jnp.concatenate([lower_half * cos_tab - upper_half * sin_tab, upper_half * cos_tab + lower_half * sin_tab], axis=-1).astype(jnp.bfloat16)


def swiglu(gate_val, up_val):
    return (jax.nn.silu(gate_val.astype(jnp.float32)) * up_val.astype(jnp.float32)).astype(jnp.bfloat16)


def attention(qkv_seq, rope_cos, rope_sin):
    queries = rotate(qkv_seq[:, :, :GROUP_SIZE, :], rope_cos[:, None, None, :], rope_sin[:, None, None, :])
    key_rot = rotate(qkv_seq[:, :, GROUP_SIZE, :], rope_cos[:, None, :], rope_sin[:, None, :])
    values = qkv_seq[:, :, GROUP_SIZE + 1, :]
    scores = jnp.einsum("qkgh,pkh->kgqp", queries.astype(jnp.float32), key_rot.astype(jnp.float32)) * HEAD ** -0.5
    causal = jnp.arange(SEQ)[:, None] >= jnp.arange(SEQ)[None, :]
    attn_probs = jax.nn.softmax(jnp.where(causal, scores, -1e30), axis=-1).astype(jnp.bfloat16)
    attn_out = jnp.einsum("kgqp,pkh->qkgh", attn_probs.astype(jnp.float32), values.astype(jnp.float32))
    return attn_out.astype(jnp.bfloat16).reshape(SEQ, HEADS * HEAD)


def reference(x_in, dy_in, norm_gain, w_qkv, w_out, w_gate, w_up, w_down, rope_cos, rope_sin):
    tokens = BATCH * SEQ
    x_rows = x_in.reshape(tokens, D).astype(jnp.float32)
    dy_rows = dy_in.reshape(tokens, D)
    normed, norm_pull = jax.vjp(lambda row_vals: row_vals * lax.rsqrt(jnp.mean(row_vals * row_vals, axis=-1, keepdims=True) + NORM_EPS) * norm_gain, x_rows)
    h_val = normed.astype(jnp.bfloat16)
    qkv_seqs = jnp.dot(h_val, w_qkv, preferred_element_type=jnp.float32).astype(jnp.bfloat16).reshape(BATCH, SEQ, KV_HEADS, GROUP_SIZE + 2, HEAD)
    attn_fn = lambda packed: attention(packed, rope_cos, rope_sin)
    attn_val = lax.map(attn_fn, qkv_seqs).reshape(tokens, HEADS * HEAD)
    gate_val = jnp.dot(h_val, w_gate, preferred_element_type=jnp.float32).astype(jnp.bfloat16)
    up_val = jnp.dot(h_val, w_up, preferred_element_type=jnp.float32).astype(jnp.bfloat16)
    act_val, act_pull = jax.vjp(swiglu, gate_val, up_val)
    mix_sum = jnp.dot(attn_val, w_out, preferred_element_type=jnp.float32) + jnp.dot(act_val, w_down, preferred_element_type=jnp.float32)
    y_out = (x_rows + mix_sum).astype(jnp.bfloat16)
    d_attn = jnp.dot(dy_rows, w_out.T, preferred_element_type=jnp.float32).astype(jnp.bfloat16)
    d_act = jnp.dot(dy_rows, w_down.T, preferred_element_type=jnp.float32).astype(jnp.bfloat16)
    d_gate, d_up = act_pull(d_act)

    def seq_grad(seq_pair):
        seq_pull = jax.vjp(attn_fn, seq_pair[0])[1]
        return seq_pull(seq_pair[1])[0]

    d_qkv = lax.map(seq_grad, (qkv_seqs, d_attn.reshape(BATCH, SEQ, HEADS * HEAD))).reshape(tokens, QKV_COLS)
    d_h = (jnp.dot(d_qkv, w_qkv.T, preferred_element_type=jnp.float32) + jnp.dot(d_gate, w_gate.T, preferred_element_type=jnp.float32) + jnp.dot(d_up, w_up.T, preferred_element_type=jnp.float32)).astype(jnp.bfloat16)
    dx_rows = (dy_rows.astype(jnp.float32) + norm_pull(d_h.astype(jnp.float32))[0]).astype(jnp.bfloat16)
    return (
        y_out.reshape(BATCH, SEQ, D),
        dx_rows.reshape(BATCH, SEQ, D),
        jnp.dot(h_val.T, d_qkv, preferred_element_type=jnp.float32),
        jnp.dot(attn_val.T, dy_rows, preferred_element_type=jnp.float32),
        jnp.dot(h_val.T, d_gate, preferred_element_type=jnp.float32),
        jnp.dot(h_val.T, d_up, preferred_element_type=jnp.float32),
        jnp.dot(act_val.T, dy_rows, preferred_element_type=jnp.float32),
    )
```

```python
import functools

import jax
import jax.numpy as jnp
from jax import lax
from jax.experimental import pallas as pl
from jax.experimental.pallas import tpu as pltpu
from jax.sharding import PartitionSpec as P


NORM_EPS = 1e-5
ROW_BLOCK = 256
CUT_LANES, CUT_TOTAL = 19, 37


def norm_fwd(row_vals, norm_gain):
    return row_vals * lax.rsqrt(jnp.mean(row_vals * row_vals, axis=-1, keepdims=True) + NORM_EPS) * norm_gain


def swiglu(gate_val, up_val):
    return (jax.nn.silu(gate_val.astype(jnp.float32)) * up_val.astype(jnp.float32)).astype(jnp.bfloat16)


def dot_nn(lhs, rhs):
    return lax.dot_general(lhs, rhs, (((1,), (0,)), ((), ())), preferred_element_type=jnp.float32)


def dot_nt(lhs, rhs):
    return lax.dot_general(lhs, rhs, (((1,), (1,)), ((), ())), preferred_element_type=jnp.float32)


def dot_tn(lhs, rhs):
    return lax.dot_general(lhs, rhs, (((0,), (0,)), ((), ())), preferred_element_type=jnp.float32)


def after(value, *earlier):
    return lax.optimization_barrier((value, earlier))[0]


def attention_kernel(group_size, q_ref, k_ref, v_ref, do_ref, cos_ref, sin_ref, o_ref, dqkv_ref, k_rot, dk_acc, dv_acc):
    head = pl.program_id(1)
    seq_len, head_dim = q_ref.shape
    scale = head_dim ** -0.5

    def turn(tensor, sign):
        wide = tensor.astype(jnp.float32)
        return (wide * cos_ref[...] + pltpu.roll(wide, head_dim // 2, 1) * (sin_ref[...] * sign)).astype(jnp.bfloat16)

    @pl.when(head == 0)
    def _():
        k_rot[...] = turn(k_ref[...], 1.0)
        dk_acc[...] = jnp.zeros_like(dk_acc)
        dv_acc[...] = jnp.zeros_like(dv_acc)

    q_rot = turn(q_ref[...], 1.0)
    dq_blocks = []
    for block in range(seq_len // ROW_BLOCK):
        rows = slice(block * ROW_BLOCK, (block + 1) * ROW_BLOCK)
        width = (block + 1) * ROW_BLOCK
        q_blk = q_rot[rows, :]
        do_blk = do_ref[rows, :]
        scores = dot_nt(q_blk, k_rot[:width, :]) * scale
        row_pos = lax.broadcasted_iota(jnp.int32, (ROW_BLOCK, width), 0) + block * ROW_BLOCK
        col_pos = lax.broadcasted_iota(jnp.int32, (ROW_BLOCK, width), 1)
        scores = jnp.where(row_pos >= col_pos, scores, -1e30)
        weights = jnp.exp(scores - jnp.max(scores, axis=-1, keepdims=True))
        probs = weights / jnp.sum(weights, axis=-1, keepdims=True)
        probs_b = probs.astype(jnp.bfloat16)
        o_ref[rows, :] = dot_nn(probs_b, v_ref[:width, :]).astype(jnp.bfloat16)
        d_probs = dot_nt(do_blk, v_ref[:width, :]).astype(jnp.bfloat16).astype(jnp.float32)
        inner = jnp.sum(probs * d_probs, axis=-1, keepdims=True)
        d_scores = (probs * (d_probs - inner) * scale).astype(jnp.bfloat16)
        dq_blocks.append(dot_nn(d_scores, k_rot[:width, :]))
        dk_acc[:width, :] += dot_tn(d_scores, q_blk)
        dv_acc[:width, :] += dot_tn(probs_b, do_blk)
    dq = jnp.concatenate(dq_blocks, axis=0).astype(jnp.bfloat16)
    dqkv_ref[:, pl.ds(pl.multiple_of(head * head_dim, head_dim), head_dim)] = turn(dq, -1.0)

    @pl.when(head == group_size - 1)
    def _():
        dqkv_ref[:, group_size * head_dim:(group_size + 1) * head_dim] = turn(dk_acc[...].astype(jnp.bfloat16), -1.0)
        dqkv_ref[:, (group_size + 1) * head_dim:] = dv_acc[...].astype(jnp.bfloat16)


def attention_grads(qkv_val, d_attn, rope_cos, rope_sin, seq_len):
    tokens, qkv_cols = qkv_val.shape
    head_dim = 2 * rope_cos.shape[1]
    group_size = d_attn.shape[1] // head_dim
    seqs = tokens // seq_len
    cos_full = jnp.concatenate([rope_cos, rope_cos], axis=1)
    sin_full = jnp.concatenate([-rope_sin, rope_sin], axis=1)
    head_spec = pl.BlockSpec((seq_len, head_dim), lambda s, h: (s, h))
    table_spec = pl.BlockSpec((seq_len, head_dim), lambda s, h: (0, 0))
    return pl.pallas_call(
        functools.partial(attention_kernel, group_size),
        grid=(seqs, group_size),
        in_specs=[
            head_spec,
            pl.BlockSpec((seq_len, head_dim), lambda s, h: (s, group_size)),
            pl.BlockSpec((seq_len, head_dim), lambda s, h: (s, group_size + 1)),
            head_spec,
            table_spec,
            table_spec,
        ],
        out_specs=[head_spec, pl.BlockSpec((seq_len, qkv_cols), lambda s, h: (s, 0))],
        out_shape=[
            jax.ShapeDtypeStruct(d_attn.shape, jnp.bfloat16),
            jax.ShapeDtypeStruct(qkv_val.shape, jnp.bfloat16),
        ],
        scratch_shapes=[
            pltpu.VMEM((seq_len, head_dim), jnp.bfloat16),
            pltpu.VMEM((seq_len, head_dim), jnp.float32),
            pltpu.VMEM((seq_len, head_dim), jnp.float32),
        ],
        compiler_params=pltpu.CompilerParams(dimension_semantics=("arbitrary", "arbitrary"), vmem_limit_bytes=40 * 2**20),
        cost_estimate=pl.CostEstimate(flops=seqs * group_size * seq_len * seq_len * head_dim * 24, bytes_accessed=2 * 2 * (qkv_val.size + d_attn.size), transcendentals=seqs * group_size * seq_len * seq_len),
        name="attention_grads",
    )(qkv_val, qkv_val, qkv_val, d_attn, cos_full, sin_full)


def solution(mesh):
    act_spec = P("fsdp", "model", None)
    col_spec = P("fsdp", "model")
    row_spec = P("model", "fsdp")

    def swap(value):
        return lax.ppermute(value, "fsdp", [(0, 1), (1, 0)])

    def layer_body(x_in, dy_in, norm_gain, w_qkv, w_out, w_gate, w_up, w_down, rope_cos, rope_sin):
        me = lax.axis_index("fsdp")
        half = w_qkv.shape[0]
        batch_loc = x_in.shape[0]
        seq_len = rope_cos.shape[0]
        ffn = w_gate.shape[1]

        def halves(value):
            return [lax.dynamic_slice_in_dim(value, side * half, half, axis=2) for side in (me, 1 - me)]

        def join(own, other):
            return jnp.where(me == 0, jnp.concatenate([own, other], axis=2), jnp.concatenate([other, own], axis=2))

        def all_tokens(value):
            own, other = halves(value)
            peer_own = swap(other)
            peer_other = swap(own)
            full_own = lax.all_gather(jnp.concatenate([own, peer_own], axis=0), "model", axis=1, tiled=True)
            full_other = lax.all_gather(jnp.concatenate([other, peer_other], axis=0), "model", axis=1, tiled=True)
            return full_own.reshape(-1, half), full_other.reshape(-1, half)

        x_rows = x_in.astype(jnp.float32)
        normed, norm_pull = jax.vjp(lambda row_vals: norm_fwd(row_vals, norm_gain), x_rows)
        h_own, h_oth = all_tokens(normed.astype(jnp.bfloat16))
        dy_own, dy_oth = all_tokens(dy_in)
        cut = CUT_LANES * (ffn // CUT_TOTAL)
        weights = {
            "wqkv": w_qkv, "wout": w_out,
            "gate0": w_gate[:, :cut], "up0": w_up[:, :cut], "down0": w_down[:cut, :],
            "gate1": w_gate[:, cut:], "up1": w_up[:, cut:], "down1": w_down[cut:, :],
        }
        peers = {}
        for name, weight in weights.items():
            peers[name] = swap(weight)

        gate0_own = dot_nn(h_own, weights["gate0"])
        up0_own = dot_nn(h_own, weights["up0"])
        qkv_val = (dot_nn(h_own, w_qkv) + dot_nn(h_oth, after(peers["wqkv"], gate0_own, up0_own))).astype(jnp.bfloat16)
        h_late = after(h_own, qkv_val)
        gate1_own = dot_nn(h_late, weights["gate1"])
        up1_own = dot_nn(h_late, weights["up1"])
        dy_late = after(dy_own, gate1_own, up1_own)
        down0_own = dot_nt(dy_late, weights["down0"])
        d_attn = (dot_nt(dy_late, w_out) + dot_nt(dy_oth, after(peers["wout"], down0_own))).astype(jnp.bfloat16)
        attn_val, d_qkv = attention_grads(qkv_val, d_attn, rope_cos, rope_sin, seq_len)

        gate0 = (gate0_own + dot_nn(h_oth, after(peers["gate0"], d_qkv))).astype(jnp.bfloat16)
        attn_late, d_qkv_late = after((attn_val, d_qkv), gate0)
        part_sum = dot_nn(attn_late, w_out)
        dh_part = dot_nt(d_qkv_late, w_qkv)
        dw_out = dot_tn(attn_late, dy_own)
        dw_qkv = dot_tn(h_own, d_qkv_late)
        up0 = (up0_own + dot_nn(h_oth, after(peers["up0"], part_sum, dh_part, dw_out, dw_qkv))).astype(jnp.bfloat16)
        act0, act0_pull = jax.vjp(swiglu, gate0, up0)
        part_sum = part_sum + dot_nn(act0, weights["down0"])
        dw_down0 = dot_tn(act0, dy_own)
        down1_own = dot_nt(after(dy_own, part_sum, dw_down0), weights["down1"])
        d_act0 = (down0_own + dot_nt(dy_oth, after(peers["down0"], down1_own))).astype(jnp.bfloat16)
        d_gate0, d_up0 = act0_pull(d_act0)
        dh_part = dh_part + dot_nt(d_gate0, weights["gate0"]) + dot_nt(d_up0, weights["up0"])

        gate1 = (gate1_own + dot_nn(h_oth, after(peers["gate1"], dh_part))).astype(jnp.bfloat16)
        up1 = (up1_own + dot_nn(h_oth, after(peers["up1"], gate1))).astype(jnp.bfloat16)
        act1, act1_pull = jax.vjp(swiglu, gate1, up1)
        part_sum = part_sum + dot_nn(act1, weights["down1"])
        act_late = after((act0, act1), part_sum)
        dw_down = dot_tn(jnp.concatenate(act_late, axis=1), dy_own)
        d_act1 = (down1_own + dot_nt(dy_oth, after(peers["down1"], dw_down))).astype(jnp.bfloat16)
        d_gate1, d_up1 = act1_pull(d_act1)
        mix_sum = lax.psum_scatter(part_sum.reshape(2 * batch_loc, seq_len, half), "model", scatter_dimension=1, tiled=True)
        mid = batch_loc * seq_len
        gate1_late, up1_late = after((weights["gate1"], weights["up1"]), mix_sum)
        dh_peer = dh_part[mid:] + dot_nt(d_gate1[mid:], gate1_late) + dot_nt(d_up1[mid:], up1_late)
        gate1_late, up1_late = after((gate1_late, up1_late), dh_peer)
        dh_mine = dh_part[:mid] + dot_nt(d_gate1[:mid], gate1_late) + dot_nt(d_up1[:mid], up1_late)
        h_last, gates_last, ups_last = after((h_own, (d_gate0, d_gate1), (d_up0, d_up1)), dh_mine)
        dw_gate = dot_tn(h_last, jnp.concatenate(gates_last, axis=1))
        dw_up = dot_tn(h_last, jnp.concatenate(ups_last, axis=1))

        mix_oth = swap(mix_sum[batch_loc:])
        y_out = (x_rows + join(mix_sum[:batch_loc], mix_oth)).astype(jnp.bfloat16)
        d_h_peer = lax.psum_scatter(dh_peer.reshape(batch_loc, seq_len, half), "model", scatter_dimension=1, tiled=True).astype(jnp.bfloat16)
        d_h_mine = lax.psum_scatter(dh_mine.reshape(batch_loc, seq_len, half), "model", scatter_dimension=1, tiled=True).astype(jnp.bfloat16)
        d_h_oth = swap(d_h_peer)
        d_h = join(d_h_mine, d_h_oth)
        dx_out = (dy_in.astype(jnp.float32) + norm_pull(d_h.astype(jnp.float32))[0]).astype(jnp.bfloat16)
        return (
            y_out,
            dx_out,
            dw_qkv,
            dw_out,
            dw_gate,
            dw_up,
            dw_down,
        )

    return jax.shard_map(
        layer_body,
        mesh=mesh,
        in_specs=(act_spec, act_spec, P(), col_spec, row_spec, col_spec, col_spec, row_spec, P(), P()),
        out_specs=(act_spec, act_spec, col_spec, row_spec, col_spec, col_spec, row_spec),
        check_vma=False,
    )
```
